32 devices in a mesh: col: 8 (over y, x, core), row: 4 (over z).
Axes of the slice: x: 2, y: 2, z: 4, core: 2. Of those that a mesh axis runs over, the one named last changes fastest.
Arguments:
- rhs: float32 [2, 32, 4, 4096], P(None, None, 'row', 'col'), may hold values from -6 to 6
- u_factor: bfloat16 [64, 40, 2, 256, 128], P('row', 'col'), may hold values from -0.078125 to 0.078125
- v_factor: bfloat16 [64, 40, 2, 256, 128], P('row', 'col'), may hold values from -0.375 to 0.375
- ranks: int32 [64, 40], P('row', 'col'), may hold values from 8 to 128, as said below
- assign: int32 [40], replicated, may hold values from 0 to 39, each once
Outputs:
- solution: float32 [2, 32, 10240], P(None, None, 'col')
- residual_estimate: float32 [32], replicated
The draws below stay inside these ranges and needn't reach their ends.
Inputs may be any that keep to these rules, and one draw needn't show every extreme that they name: `ranks`: every entry is 128 // 16 times a power of two from 1 to 16.
All inputs are finite; a program needn't handle non-finite values.
Results may differ from the reference program's by a relative error of at most 0.0068.
Values may be sent and summed in bfloat16 or wider, within the bound.
No kernel may reach another device: no remote copies, remote signals or barrier semaphores. Data moves between devices by JAX's collectives and lax.ppermute only.
A program may use at most 128 MiB of HBM per device.

```python
import jax
import jax.numpy as jnp
from jax import lax

NB = 256
RMAX = 128
NS = 32
ITERS = 2
TR = 64
TC = 40
MR = 4096
N_ROW = 4


def draw_ranks(key, part):
    first = jax.random.randint(jax.random.fold_in(key, 11), (TR, TC), 0, 5)
    second = jax.random.randint(jax.random.fold_in(key, 12), (TR, TC), 0, 5)
    level = jnp.minimum(first, second)
    values = RMAX // 16 * jnp.left_shift(jnp.ones_like(level), level)
    values = values.at[0, 0].set(RMAX).at[0, 1].set(RMAX // 16)
    return values.astype(jnp.int32)


def level_of(rng, shape, cuts, smallest, high):
    factor_of = 1.0
    for position, shards_of in cuts:
        draws = jax.random.uniform(jax.random.fold_in(jax.random.fold_in(rng, 6), position), (shards_of,), jnp.float32, smallest / len(cuts), high / len(cuts))
        factor_of = factor_of * jnp.repeat(jnp.exp(draws), shape[position] // shards_of).reshape((-1,) + (1,) * (len(shape) - 1 - position))
    return factor_of


def noise(own_key, shape, spread, limit, split=(), kind=jnp.bfloat16):
    level = level_of(own_key, shape, split, -0.22, 0.18) if split else 1.0
    array = jax.random.normal(own_key, shape, jnp.float32) * spread * level
    return jnp.minimum(jnp.maximum(array, -limit), limit).astype(kind)


def setup_inputs(seed: int = 0) -> dict:
    key_of = jax.random.split(jax.random.key(seed), 6)
    return {
        "rhs": noise(key_of[0], (2, NS, N_ROW, MR), 1.0, 6.0, ((2, 4), (3, 8)), jnp.float32),
        "u_factor": noise(key_of[1], (TR, TC, 2, NB, RMAX), (RMAX * TC) ** -0.5, 0.078125, ((0, 4), (1, 8))),
        "v_factor": noise(key_of[2], (TR, TC, 2, NB, RMAX), NB ** -0.5, 0.375, ((0, 4), (1, 8))),
        "ranks": draw_ranks(jax.random.fold_in(key_of[5], 71), 0),
        "assign": jax.random.permutation(key_of[4], TC).astype(jnp.int32),
    }


HIGH = lax.Precision.HIGHEST

def rounded(value):
    return lax.optimization_barrier(value.astype(jnp.bfloat16)).astype(jnp.float32)

def sum_squares(value):
    return lax.optimization_barrier(jnp.sum(value * value, axis=(0, 2)))

def reference(rhs, u_factor, v_factor, ranks, assign):
    tile_rows, tile_cols = ranks.shape
    tile_size = u_factor.shape[3]
    rank_cap = u_factor.shape[4]
    sources = rhs.shape[1]
    rank_iota = lax.broadcasted_iota(jnp.int32, (tile_rows, tile_cols, 1, 1, rank_cap), 4)
    mask = (rank_iota < ranks[:, :, None, None, None]).astype(jnp.float32)

    def forward(model_vec):
        model_b = rounded(model_vec).reshape(2, sources, tile_cols, tile_size)

        def one_row(packed):
            left, right, mask_row = packed
            raw = jnp.einsum('pcnk,dspn->pcdsk', right.astype(jnp.float32), model_b, precision=HIGH)
            coeff = jnp.stack([raw[:, 0, 0] - raw[:, 1, 1], raw[:, 0, 1] + raw[:, 1, 0]], axis=1) * mask_row
            coeff = rounded(coeff)
            prod = jnp.einsum('pcnk,pdsk->cdsn', left.astype(jnp.float32), coeff, precision=HIGH)
            return jnp.stack([prod[0, 0] - prod[1, 1], prod[0, 1] + prod[1, 0]], axis=0)
        blocks = lax.map(one_row, (u_factor, v_factor, mask))
        return jnp.transpose(blocks, (1, 2, 0, 3)).reshape(2, sources, tile_rows * tile_size)

    def adjoint(data_vec):
        data_b = rounded(data_vec).reshape(2, sources, tile_rows, tile_size)
        data_b = jnp.transpose(data_b, (2, 0, 1, 3))

        def one_row(carry, packed):
            left, right, mask_row, data_row = packed
            raw = jnp.einsum('pcnk,dsn->pcdsk', left.astype(jnp.float32), data_row, precision=HIGH)
            coeff = jnp.stack([raw[:, 0, 0] + raw[:, 1, 1], raw[:, 0, 1] - raw[:, 1, 0]], axis=1) * mask_row
            coeff = rounded(coeff)
            prod = jnp.einsum('pcnk,pdsk->cdspn', right.astype(jnp.float32), coeff, precision=HIGH)
            part = jnp.stack([prod[0, 0] + prod[1, 1], prod[0, 1] - prod[1, 0]], axis=0)
            return (carry + part, None)
        start = jnp.zeros((2, sources, tile_cols, tile_size), jnp.float32)
        total, _ = lax.scan(one_row, start, (u_factor, v_factor, mask, data_b))
        return total.reshape(2, sources, tile_cols * tile_size)
    data_hat = rhs.reshape(2, sources, tile_rows * tile_size)
    beta_now = jnp.sqrt(sum_squares(data_hat))
    u_vec = data_hat / beta_now[None, :, None]
    v_hat = adjoint(data_hat) / beta_now[None, :, None]
    alpha_now = jnp.sqrt(sum_squares(v_hat))
    v_vec = v_hat / alpha_now[None, :, None]
    w_vec = v_vec
    x_vec = jnp.zeros_like(v_vec)
    phibar = beta_now
    rhobar = alpha_now
    for iteration in range(ITERS):
        data_hat = forward(v_vec) - alpha_now[None, :, None] * u_vec
        beta_now = jnp.sqrt(sum_squares(data_hat))
        u_vec = data_hat / beta_now[None, :, None]
        v_hat = adjoint(data_hat) / beta_now[None, :, None] - beta_now[None, :, None] * v_vec
        alpha_now = jnp.sqrt(sum_squares(v_hat))
        v_vec = v_hat / alpha_now[None, :, None]
        rho_now = jnp.sqrt(rhobar * rhobar + beta_now * beta_now)
        cosine = rhobar / rho_now
        sine = beta_now / rho_now
        theta = sine * alpha_now
        rhobar = -cosine * alpha_now
        phi_now = cosine * phibar
        phibar = sine * phibar
        x_vec = x_vec + (phi_now / rho_now)[None, :, None] * w_vec
        w_vec = v_vec - (theta / rho_now)[None, :, None] * w_vec
    inverse = jnp.zeros((tile_cols,), jnp.int32).at[assign].set(jnp.arange(tile_cols, dtype=jnp.int32))
    natural = x_vec.reshape(2, sources, tile_cols, tile_size)[:, :, inverse]
    return (natural.reshape(2, sources, tile_cols * tile_size), phibar)
```

```python
import functools

import jax
import jax.numpy as jnp
from jax import lax
from jax.experimental import pallas as pl
from jax.experimental.pallas import tpu as pltpu
from jax.sharding import PartitionSpec as P

F32 = jnp.float32
BF16 = jnp.bfloat16
EXT = 128
VMEM = pl.BlockSpec(memory_space=pltpu.VMEM)
SMEM = pl.BlockSpec(memory_space=pltpu.SMEM)
PARAMS = pltpu.CompilerParams(vmem_limit_bytes=48 * 1024 * 1024)


def lanes_of(columns, rows):
    lane = lax.broadcasted_iota(jnp.int32, (rows, EXT), 1)
    out = jnp.zeros((rows, EXT), F32)
    for number, column in enumerate(columns):
        rest = column
        for term in range(3):
            part = rest.astype(BF16).astype(F32)
            rest = rest - part
            out = jnp.where(lane == 3 * number + term, part, out)
    return out.astype(BF16)


def column_of(ext, number):
    lane = lax.broadcasted_iota(jnp.int32, ext.shape, 1)
    chosen = (lane >= 3 * number) & (lane < 3 * number + 3)
    return jnp.sum(jnp.where(chosen, ext, 0.0), axis=1, keepdims=True)


def both_parts(column, half):
    real, imag = parts_of(column, half)
    return join(real + imag, real + imag)


def parts_of(raw, half):
    rows, width = raw.shape
    split = raw.reshape(rows // (2 * half), 2, half, width)
    return split[:, 0], split[:, 1]


def join(first, second):
    groups, half, width = first.shape
    return jnp.stack([first, second], axis=1).reshape(groups * 2 * half, width)


def tile_coeff(vec, tile, rank, conj, half):
    k = tile.shape[2]
    raw = jnp.dot(vec, jnp.concatenate([tile[0], tile[1]], axis=1), preferred_element_type=F32)
    rr, ri = parts_of(raw[:, :k], half)
    ir, ii = parts_of(raw[:, k:], half)
    if conj:
        real, imag = rr + ii, ri - ir
    else:
        real, imag = rr - ii, ri + ir
    lane = lax.broadcasted_iota(jnp.int32, real.shape, 2)
    real = jnp.where(lane < rank, real, 0.0)
    imag = jnp.where(lane < rank, imag, 0.0)
    if conj:
        left = jnp.concatenate([join(real, imag), join(imag, -real)], axis=1)
    else:
        left = jnp.concatenate([join(real, imag), join(-imag, real)], axis=1)
    return left.astype(BF16)


def expand(left, tile):
    right = jnp.concatenate([tile[0], tile[1]], axis=1)
    return lax.dot_general(left, right, (((1,), (1,)), ((), ())), preferred_element_type=F32)


def adjoint_body(n_col, n_row, place, ranks, u_ref, v_ref, *refs):
    pieces, outs, (d_scr, z_scr) = refs[:n_col], refs[n_col : n_col + n_row], refs[n_col + n_row :]
    step = pl.program_id(0)
    tile_cols, tile_size = u_ref.shape[1], u_ref.shape[3]
    local = pieces[0].shape[1] - EXT

    @pl.when(step == 0)
    def _():
        z_scr[...] = jnp.zeros_like(z_scr)
        for j, piece in enumerate(pieces):
            held = jnp.bitwise_xor(place[0], j)
            if local >= tile_size:
                for w in range(local // tile_size):
                    d_scr[held * (local // tile_size) + w] = piece[:, w * tile_size : (w + 1) * tile_size]
            else:
                share = tile_size // local
                d_scr[held // share, :, pl.ds(pl.multiple_of((held % share) * local, local), local)] = piece[:, :local]

    data = d_scr[step]
    for p in range(tile_cols):
        left = tile_coeff(data, u_ref[0, p], ranks[step, p], True, data.shape[0] // (2 * n_row))
        z_scr[:, p * tile_size : (p + 1) * tile_size] += expand(left, v_ref[0, p])

    @pl.when(step == pl.num_programs(0) - 1)
    def _():
        width = tile_cols * tile_size
        ext = sum(piece[:, local:].astype(F32) for piece in pieces)
        ext = lanes_of([column_of(ext, 0)], ext.shape[0])
        for k, out in enumerate(outs):
            rows = out.shape[0]
            out[:, :width] = z_scr[k * rows : (k + 1) * rows, :].astype(BF16)
            out[:, width:] = ext[k * rows : (k + 1) * rows, :]


def forward_body(n_col, n_row, place, ranks, u_ref, v_ref, *refs):
    pieces, outs, (x_scr, y_scr) = refs[:n_row], refs[n_row : n_row + n_col], refs[n_row + n_col :]
    step = pl.program_id(0)
    tile_cols, tile_size = u_ref.shape[1], u_ref.shape[3]
    width = tile_cols * tile_size

    @pl.when(step == 0)
    def _():
        for k, piece in enumerate(pieces):
            rows = piece.shape[0]
            x_scr[k * rows : (k + 1) * rows, :] = piece[...]

    total = None
    for p in range(tile_cols):
        model = x_scr[:, p * tile_size : (p + 1) * tile_size]
        left = tile_coeff(model, v_ref[0, p], ranks[step, p], False, model.shape[0] // (2 * n_row))
        term = expand(left, u_ref[0, p])
        total = term if total is None else total + term
    y_scr[step] = total.astype(BF16)

    @pl.when(step == pl.num_programs(0) - 1)
    def _():
        for j, out in enumerate(outs):
            local = out.shape[1] - EXT
            held = jnp.bitwise_xor(place[0], j)
            if local >= tile_size:
                for w in range(local // tile_size):
                    out[:, w * tile_size : (w + 1) * tile_size] = y_scr[held * (local // tile_size) + w]
            else:
                share = tile_size // local
                out[:, :local] = y_scr[held // share, :, pl.ds(pl.multiple_of((held % share) * local, local), local)]
            out[:, local:] = x_scr[:, width:]


def product(body, place, ranks, u_factor, v_factor, pieces, out_shapes, scratch):
    tile_rows, tile_cols, _, tile_size, rank_cap = u_factor.shape
    block = pl.BlockSpec((1, tile_cols, 2, tile_size, rank_cap), lambda i, *_: (i, 0, 0, 0, 0))
    whole = lambda shape: pl.BlockSpec(shape, lambda i, *_: (0,) * len(shape))
    return pl.pallas_call(
        body,
        grid_spec=pltpu.PrefetchScalarGridSpec(
            num_scalar_prefetch=2,
            grid=(tile_rows,),
            in_specs=[block, block] + [whole(piece.shape) for piece in pieces],
            out_specs=[whole(shape.shape) for shape in out_shapes],
            scratch_shapes=scratch,
        ),
        out_shape=out_shapes,
        compiler_params=PARAMS,
    )(place, ranks, u_factor, v_factor, *pieces)


def small(body, out_shapes, *args):
    return pl.pallas_call(
        body,
        in_specs=[SMEM if arg.dtype == jnp.int32 else VMEM for arg in args],
        out_specs=[VMEM] * len(out_shapes),
        out_shape=out_shapes,
        compiler_params=PARAMS,
    )(*args)


def total_of(refs, rows, columns):
    return sum(ref[rows, columns].astype(F32) for ref in refs)


def begin_body(n_row, place, rhs, data, payload):
    rows, local = data.shape
    half = rows // (2 * n_row)
    for k in range(n_row):
        held = jnp.bitwise_xor(place[1], k)
        for part in range(2):
            at = (2 * k + part) * half
            data[at : at + half, :] = rhs[part, pl.ds(pl.multiple_of(held * half, half), half), :]
    values = data[...]
    payload[:, :local] = values.astype(BF16)
    payload[:, local:] = lanes_of([jnp.sum(values * values, axis=1, keepdims=True)], rows)


def model_first_body(n_row, *refs):
    pieces, (v_hat, payload) = refs[:n_row], refs[n_row:]
    width = v_hat.shape[1]
    total = total_of(pieces, slice(None), slice(0, width))
    beta2 = both_parts(column_of(total_of(pieces, slice(None), slice(width, None)), 0), total.shape[0] // 2)
    value = total / jnp.sqrt(beta2)
    v_hat[...] = value
    payload[:, :width] = value.astype(BF16)
    payload[:, width:] = lanes_of([beta2, jnp.sum(value * value, axis=1, keepdims=True)], value.shape[0])


def model_next_body(n_row, v_prev, scalars, *refs):
    pieces, (payload,) = refs[:n_row], refs[n_row:]
    rows, width = v_prev.shape
    total = total_of(pieces, slice(None), slice(0, width))
    beta2 = both_parts(column_of(total_of(pieces, slice(None), slice(width, None)), 0), total.shape[0] // 2)
    beta = jnp.sqrt(beta2)
    alpha_prev = scalars[:rows, 0:1]
    value = total / beta - (beta / alpha_prev) * v_prev[...]
    payload[:, :width] = value.astype(BF16)
    payload[:, width:] = lanes_of([beta2, jnp.sum(value * value, axis=1, keepdims=True)], rows)


def scalars_of(pieces, local, n_col, n_row):
    ext = total_of(pieces, slice(None), slice(local, None))
    beta = jnp.sqrt(column_of(ext, 0) * (1.0 / n_col))
    alpha = jnp.sqrt(both_parts(column_of(ext, 1), ext.shape[0] // (2 * n_row)))
    return alpha, beta


def data_next_body(n_col, n_row, data_prev, *refs):
    pieces, (data, payload, scalars) = refs[:n_col], refs[n_col:]
    rows, local = data_prev.shape
    alpha, beta = scalars_of(pieces, local, n_col, n_row)
    value = total_of(pieces, slice(None), slice(0, local)) / alpha - (alpha / beta) * data_prev[...]
    data[...] = value
    payload[:, :local] = value.astype(BF16)
    payload[:, local:] = lanes_of([jnp.sum(value * value, axis=1, keepdims=True)], rows)
    lane = lax.broadcasted_iota(jnp.int32, scalars.shape, 1)
    scalars[...] = jnp.where(lane == 0, alpha, beta)


def data_last_body(n_col, n_row, data_prev, *refs):
    pieces, (square, scalars) = refs[:n_col], refs[n_col:]
    rows, local = data_prev.shape
    alpha, beta = scalars_of(pieces, local, n_col, n_row)
    value = total_of(pieces, slice(None), slice(0, local)) / alpha - (alpha / beta) * data_prev[...]
    square[...] = jnp.broadcast_to(jnp.sum(value * value, axis=1, keepdims=True), square.shape)
    lane = lax.broadcasted_iota(jnp.int32, scalars.shape, 1)
    scalars[...] = jnp.where(lane == 0, alpha, beta)


def add_body(*refs):
    refs[-1][...] = sum(ref[...] for ref in refs[:-1])


def pick_body(n_col, place, where, *refs):
    firsts, seconds, (out, scr) = refs[:n_col], refs[n_col : 2 * n_col], refs[2 * n_col :]
    rows = firsts[0].shape[0]
    width = out.shape[1]
    tile_cols = where.shape[0]
    tile = width // tile_cols
    for j in range(n_col):
        scr[j, :rows] = firsts[j][:, :width]
        scr[j, rows:] = seconds[j][:, :width]
    for p in range(tile_cols):
        held = where[p]
        source = jnp.bitwise_xor(held // tile_cols, place[0])
        at = pl.multiple_of((held % tile_cols) * tile, tile)
        out[:, p * tile : (p + 1) * tile] = scr[source, :, pl.ds(at, tile)]


def finish_body(n_row, place, *refs):
    squares, pieces = refs[:n_row], refs[n_row : 2 * n_row]
    scal_first, scal_next, solution, residual = refs[2 * n_row :]
    rows = squares[0].shape[0]
    total = squares[0][...]
    for k in range(1, n_row):
        other = squares[k][...].reshape(n_row, rows // n_row, squares[k].shape[1])
        moved = jnp.stack([other[g ^ k] for g in range(n_row)], axis=0)
        total = total + moved.reshape(total.shape)
    half = rows // (2 * n_row)
    beta_last = jnp.sqrt(both_parts(total[:, 0:1], half))
    alpha_0, beta_0 = scal_first[:, 0:1], scal_first[:, 1:2]
    alpha_1, beta_1 = scal_next[:, 0:1], scal_next[:, 1:2]
    rho = jnp.sqrt(alpha_0 * alpha_0 + beta_1 * beta_1)
    cosine = alpha_0 / rho
    sine = beta_1 / rho
    theta = sine * alpha_1
    rhobar = -cosine * alpha_1
    phi = cosine * beta_0
    phibar = sine * beta_0
    first = phi / rho
    slope = theta / rho
    rho = jnp.sqrt(rhobar * rhobar + beta_last * beta_last)
    second = (rhobar / rho) * phibar / rho
    phibar = (beta_last / rho) * phibar
    weight_0 = (first - second * slope) / alpha_0
    weight_1 = second / alpha_1
    for k in range(n_row):
        held = jnp.bitwise_xor(place[1], k)
        at = pl.multiple_of(held * half, half)
        lo, hi = 2 * half * k, 2 * half * (k + 1)
        v_0 = pieces[k][: 2 * half, :].astype(F32)
        v_1 = pieces[k][2 * half :, :].astype(F32)
        mixed = weight_0[lo:hi] * v_0 + weight_1[lo:hi] * v_1
        for part in range(2):
            solution[part, pl.ds(at, half), :] = mixed[part * half : (part + 1) * half]
        residual[pl.ds(at, half), :] = jnp.broadcast_to(phibar[lo : lo + half], (half, residual.shape[1]))


def swap(value, axis, size, mask):
    return lax.ppermute(value, axis, [(j, j ^ mask) for j in range(size)])


def scatter(pieces, axis, size):
    return [pieces[0]] + [swap(pieces[k], axis, size, k) for k in range(1, size)]


def gather_row(value, size):
    return [value] + [swap(value, "row", size, k) for k in range(1, size)]


def gather_col(value, size):
    even = {0: value}
    for k in range(2, size, 2):
        even[k] = swap(value, "col", size, k)
    pieces = []
    for k in range(0, size, 2):
        pieces += [even[k], swap(even[k], "col", size, 1)]
    return pieces


def on_device(rhs, u_factor, v_factor, ranks, assign):
    n_col, n_row = lax.axis_size("col"), lax.axis_size("row")
    tile_rows, tile_cols, _, tile_size, _ = u_factor.shape
    sources, local = rhs.shape[1], rhs.shape[3]
    rows = 2 * sources
    share = rows // n_row
    width = tile_cols * tile_size
    place = jnp.stack([lax.axis_index("col"), lax.axis_index("row")]).astype(jnp.int32)
    shape = jax.ShapeDtypeStruct
    data_shape, model_shape = shape((rows, local + EXT), BF16), shape((share, width + EXT), BF16)
    scalar_shape = shape((rows, EXT), F32)

    adjoint = functools.partial(
        product,
        functools.partial(adjoint_body, n_col, n_row),
        place,
        ranks,
        u_factor,
        v_factor,
        out_shapes=[model_shape] * n_row,
        scratch=[pltpu.VMEM((tile_rows, rows, tile_size), BF16), pltpu.VMEM((rows, width), F32)],
    )
    forward = functools.partial(
        product,
        functools.partial(forward_body, n_col, n_row),
        place,
        ranks,
        u_factor,
        v_factor,
        out_shapes=[data_shape] * n_col,
        scratch=[pltpu.VMEM((rows, width + EXT), BF16), pltpu.VMEM((tile_rows, rows, tile_size), BF16)],
    )

    data_0, payload = small(
        functools.partial(begin_body, n_row),
        [shape((rows, local), F32), data_shape],
        place,
        rhs.reshape(2, sources, local),
    )
    partial_model = adjoint(gather_col(payload, n_col))
    v_hat_0, model_0 = small(
        functools.partial(model_first_body, n_row),
        [shape((share, width), F32), model_shape],
        *scatter(partial_model, "row", n_row),
    )
    partial_data = forward(gather_row(model_0, n_row))
    data_1, payload, scal_first = small(
        functools.partial(data_next_body, n_col, n_row),
        [shape((rows, local), F32), data_shape, scalar_shape],
        data_0,
        *scatter(partial_data, "col", n_col),
    )
    partial_model = adjoint(gather_col(payload, n_col))
    (model_1,) = small(
        functools.partial(model_next_body, n_row),
        [model_shape],
        v_hat_0,
        scal_first,
        *scatter(partial_model, "row", n_row),
    )
    partial_data = forward(gather_row(model_1, n_row))

    natural = lax.axis_index("col") * tile_cols + jnp.arange(tile_cols, dtype=jnp.int32)
    positions = jnp.arange(assign.shape[0], dtype=jnp.int32)
    where_held = jnp.sum(
        positions[None, :] * (assign[None, :] == natural[:, None]).astype(jnp.int32), axis=1
    )
    held = gather_col(model_0, n_col) + gather_col(model_1, n_col)
    picked = pl.pallas_call(
        functools.partial(pick_body, n_col),
        in_specs=[SMEM, SMEM] + [VMEM] * (2 * n_col),
        out_specs=VMEM,
        out_shape=shape((2 * share, width), BF16),
        scratch_shapes=[pltpu.VMEM((n_col, 2 * share, width), BF16)],
        compiler_params=PARAMS,
    )(place, where_held, *held)
    blocks = gather_row(picked, n_row)

    square, scal_next = small(
        functools.partial(data_last_body, n_col, n_row),
        [scalar_shape, scalar_shape],
        data_1,
        *scatter(partial_data, "col", n_col),
    )
    (square,) = small(add_body, [scalar_shape], square, swap(square, "col", n_col, 1))
    (square,) = small(
        add_body, [scalar_shape], square, *[swap(square, "col", n_col, k) for k in range(2, n_col, 2)]
    )
    solution, residual = small(
        functools.partial(finish_body, n_row),
        [shape((2, sources, width), F32), shape((sources, EXT), F32)],
        place,
        *gather_row(square, n_row),
        *blocks,
        scal_first,
        scal_next,
    )
    return (solution, residual[:, 0])


def solution(mesh):
    in_specs = (
        P(None, None, "row", "col"),
        P("row", "col", None, None, None),
        P("row", "col", None, None, None),
        P("row", "col"),
        P(),
    )
    out_specs = (P(None, None, "col"), P())
    return jax.shard_map(
        on_device, mesh=mesh, in_specs=in_specs, out_specs=out_specs, check_vma=False
    )
```

```python
import functools

import jax
import jax.numpy as jnp
from jax import lax
from jax.experimental import pallas as pl
from jax.experimental.pallas import tpu as pltpu
from jax.sharding import PartitionSpec as P

F32 = jnp.float32
BF16 = jnp.bfloat16
EXT = 128
VMEM = pl.BlockSpec(memory_space=pltpu.VMEM)
SMEM = pl.BlockSpec(memory_space=pltpu.SMEM)
UNROLL = 4
PARAMS = pltpu.CompilerParams(vmem_limit_bytes=8 * 1024 * 1024)
PRODUCT_PARAMS = pltpu.CompilerParams(vmem_limit_bytes=27 * 1024 * 1024)


def lanes_of(columns, rows):
    lane = lax.broadcasted_iota(jnp.int32, (rows, EXT), 1)
    out = jnp.zeros((rows, EXT), F32)
    for number, column in enumerate(columns):
        rest = column
        for term in range(3):
            part = rest.astype(BF16).astype(F32)
            rest = rest - part
            out = jnp.where(lane == 3 * number + term, part, out)
    return out.astype(BF16)


def column_of(ext, number):
    lane = lax.broadcasted_iota(jnp.int32, ext.shape, 1)
    chosen = (lane >= 3 * number) & (lane < 3 * number + 3)
    return jnp.sum(jnp.where(chosen, ext, 0.0), axis=1, keepdims=True)


def both_parts(column, half):
    real, imag = parts_of(column, half)
    return join(real + imag, real + imag)


def parts_of(raw, half):
    rows, width = raw.shape
    split = raw.reshape(rows // (2 * half), 2, half, width)
    return split[:, 0], split[:, 1]


def join(first, second):
    groups, half, width = first.shape
    return jnp.stack([first, second], axis=1).reshape(groups * 2 * half, width)


def tile_coeff(vec, tile, rank, conj, half):
    k = tile.shape[2]
    raw = jnp.dot(vec, jnp.concatenate([tile[0], tile[1]], axis=1), preferred_element_type=F32)
    rr, ri = parts_of(raw[:, :k], half)
    ir, ii = parts_of(raw[:, k:], half)
    if conj:
        real, imag = rr + ii, ri - ir
    else:
        real, imag = rr - ii, ri + ir
    lane = lax.broadcasted_iota(jnp.int32, real.shape, 2)
    real = jnp.where(lane < rank, real, 0.0)
    imag = jnp.where(lane < rank, imag, 0.0)
    if conj:
        left = jnp.concatenate([join(real, imag), join(imag, -real)], axis=1)
    else:
        left = jnp.concatenate([join(real, imag), join(-imag, real)], axis=1)
    return left.astype(BF16)


def expand(left, tile):
    right = jnp.concatenate([tile[0], tile[1]], axis=1)
    return lax.dot_general(left, right, (((1,), (1,)), ((), ())), preferred_element_type=F32)


def adjoint_body(n_col, n_row, stream, place, ranks, u_ref, v_ref, *refs):
    pieces, outs, rest = refs[:n_col], refs[n_col : n_col + n_row], refs[n_col + n_row :]
    tile_rows, tile_cols, _, tile_size, _ = u_ref.shape
    if stream:
        u_far, v_far, (u_ref, v_ref, d_scr, z_scr, sems) = u_ref, v_ref, rest

        def copies(i):
            return (
                pltpu.make_async_copy(u_far.at[i], u_ref.at[i], sems.at[0, i]),
                pltpu.make_async_copy(v_far.at[i], v_ref.at[i], sems.at[1, i]),
            )

        for i in range(tile_rows):
            for copy in copies(i):
                copy.start()
    else:
        d_scr, z_scr = rest
    local = pieces[0].shape[1] - EXT
    width = tile_cols * tile_size
    z_scr[...] = jnp.zeros_like(z_scr)
    for j, piece in enumerate(pieces):
        held = jnp.bitwise_xor(place[0], j)
        if local >= tile_size:
            for w in range(local // tile_size):
                d_scr[held * (local // tile_size) + w] = piece[:, w * tile_size : (w + 1) * tile_size]
        else:
            share = tile_size // local
            d_scr[held // share, :, pl.ds(pl.multiple_of((held % share) * local, local), local)] = piece[:, :local]

    def one_row(i, carry):
        if stream:
            for copy in copies(i):
                copy.wait()
        data = d_scr[i]
        half = data.shape[0] // (2 * n_row)
        lefts = [tile_coeff(data, u_ref[i, p], ranks[i, p], True, half) for p in range(tile_cols)]
        for p in range(tile_cols):
            z_scr[:, p * tile_size : (p + 1) * tile_size] += expand(lefts[p], v_ref[i, p])
        return carry

    lax.fori_loop(0, tile_rows, one_row, 0, unroll=1 if stream else UNROLL)
    ext = sum(piece[:, local:].astype(F32) for piece in pieces)
    ext = lanes_of([column_of(ext, 0)], ext.shape[0])
    for k, out in enumerate(outs):
        rows = out.shape[0]
        out[:, :width] = z_scr[k * rows : (k + 1) * rows, :].astype(BF16)
        out[:, width:] = ext[k * rows : (k + 1) * rows, :]


def forward_body(n_col, n_row, place, ranks, u_ref, v_ref, *refs):
    pieces, outs, (x_scr, y_scr) = refs[:n_row], refs[n_row : n_row + 2], refs[n_row + 2 :]
    tile_rows, tile_cols, _, tile_size, _ = u_ref.shape
    width = tile_cols * tile_size
    for k, piece in enumerate(pieces):
        rows = piece.shape[0]
        x_scr[k * rows : (k + 1) * rows, :] = piece[...]
    half = x_scr.shape[0] // (2 * n_row)

    def one_row(i, carry):
        lefts = [
            tile_coeff(x_scr[:, p * tile_size : (p + 1) * tile_size], v_ref[i, p], ranks[i, p], False, half)
            for p in range(tile_cols)
        ]
        y_scr[i] = sum(expand(lefts[p], u_ref[i, p]) for p in range(tile_cols)).astype(BF16)
        return carry

    lax.fori_loop(0, tile_rows, one_row, 0, unroll=UNROLL)
    for j in range(n_col):
        out = outs[j % 2].at[j // 2]
        local = out.shape[1] - EXT
        held = jnp.bitwise_xor(place[0], j)
        if local >= tile_size:
            for w in range(local // tile_size):
                out[:, w * tile_size : (w + 1) * tile_size] = y_scr[held * (local // tile_size) + w]
        else:
            share = tile_size // local
            out[:, :local] = y_scr[held // share, :, pl.ds(pl.multiple_of((held % share) * local, local), local)]
        out[:, local:] = x_scr[:, width:]


def product(body, place, ranks, u_factor, v_factor, pieces, out_shapes, scratch, factors=VMEM):
    return pl.pallas_call(
        body,
        in_specs=[SMEM, SMEM, factors, factors] + [VMEM] * len(pieces),
        out_specs=[VMEM] * len(out_shapes),
        out_shape=out_shapes,
        scratch_shapes=scratch,
        compiler_params=PRODUCT_PARAMS,
    )(place, ranks, u_factor, v_factor, *pieces)


def small(body, out_shapes, *args):
    return pl.pallas_call(
        body,
        in_specs=[SMEM if arg.dtype == jnp.int32 else VMEM for arg in args],
        out_specs=[VMEM] * len(out_shapes),
        out_shape=out_shapes,
        compiler_params=PARAMS,
    )(*args)


def total_of(refs, rows, columns):
    return sum(ref[rows, columns].astype(F32) for ref in refs)


def chip_body(keep, other, *outs):
    chips, rows, wide = keep.shape
    local = wide - EXT
    ext = keep[0, :, local:].astype(F32) + other[0, :, local:].astype(F32)
    ext = lanes_of([column_of(ext, 0), column_of(ext, 1)], rows)
    for k, out in enumerate(outs):
        out[:, :local] = (keep[k, :, :local].astype(F32) + other[k, :, :local].astype(F32)).astype(BF16)
        out[:, local:] = ext


def begin_body(n_row, place, rhs, data, payload):
    rows, local = data.shape
    half = rows // (2 * n_row)
    for k in range(n_row):
        held = jnp.bitwise_xor(place[1], k)
        for part in range(2):
            at = (2 * k + part) * half
            data[at : at + half, :] = rhs[part, pl.ds(pl.multiple_of(held * half, half), half), :]
    values = data[...]
    payload[:, :local] = values.astype(BF16)
    payload[:, local:] = lanes_of([jnp.sum(values * values, axis=1, keepdims=True)], rows)


def model_first_body(n_row, *refs):
    pieces, (v_hat, payload) = refs[:n_row], refs[n_row:]
    width = v_hat.shape[1]
    total = total_of(pieces, slice(None), slice(0, width))
    beta2 = both_parts(column_of(total_of(pieces, slice(None), slice(width, None)), 0), total.shape[0] // 2)
    value = total / jnp.sqrt(beta2)
    v_hat[...] = value
    payload[:, :width] = value.astype(BF16)
    payload[:, width:] = lanes_of([beta2, jnp.sum(value * value, axis=1, keepdims=True)], value.shape[0])


def model_next_body(n_row, v_prev, scalars, *refs):
    pieces, (payload, pair) = refs[:n_row], refs[n_row:]
    rows, width = v_prev.shape
    total = total_of(pieces, slice(None), slice(0, width))
    beta2 = both_parts(column_of(total_of(pieces, slice(None), slice(width, None)), 0), total.shape[0] // 2)
    beta = jnp.sqrt(beta2)
    alpha_prev = scalars[:rows, 0:1]
    value = total / beta - (beta / alpha_prev) * v_prev[...]
    payload[:, :width] = value.astype(BF16)
    payload[:, width:] = lanes_of([beta2, jnp.sum(value * value, axis=1, keepdims=True)], rows)
    pair[:rows, :] = v_prev[...].astype(BF16)
    pair[rows:, :] = value.astype(BF16)


def scalars_of(pieces, local, n_col, n_row):
    ext = total_of(pieces, slice(None), slice(local, None))
    beta = jnp.sqrt(column_of(ext, 0) * (1.0 / n_col))
    alpha = jnp.sqrt(both_parts(column_of(ext, 1), ext.shape[0] // (2 * n_row)))
    return alpha, beta


def data_next_body(n_col, n_row, data_prev, *refs):
    pieces, (data, payload, scalars) = refs[: n_col // 2], refs[n_col // 2 :]
    rows, local = data_prev.shape
    alpha, beta = scalars_of(pieces, local, n_col, n_row)
    value = total_of(pieces, slice(None), slice(0, local)) / alpha - (alpha / beta) * data_prev[...]
    data[...] = value
    payload[:, :local] = value.astype(BF16)
    payload[:, local:] = lanes_of([jnp.sum(value * value, axis=1, keepdims=True)], rows)
    lane = lax.broadcasted_iota(jnp.int32, scalars.shape, 1)
    scalars[...] = jnp.where(lane == 0, alpha, beta)


def data_last_body(n_col, n_row, data_prev, *refs):
    pieces, (square, scalars) = refs[: n_col // 2], refs[n_col // 2 :]
    rows, local = data_prev.shape
    alpha, beta = scalars_of(pieces, local, n_col, n_row)
    value = total_of(pieces, slice(None), slice(0, local)) / alpha - (alpha / beta) * data_prev[...]
    square[...] = jnp.broadcast_to(jnp.sum(value * value, axis=1, keepdims=True), square.shape)
    lane = lax.broadcasted_iota(jnp.int32, scalars.shape, 1)
    scalars[...] = jnp.where(lane == 0, alpha, beta)


def add_body(*refs):
    refs[-1][...] = sum(ref[...] for ref in refs[:-1])


def pick_body(n_col, place, where, *refs):
    pieces, (out, scr) = refs[:n_col], refs[n_col:]
    tile_cols = where.shape[0]
    tile = out.shape[1] // tile_cols
    for j in range(n_col):
        scr[j] = pieces[j][...]
    for p in range(tile_cols):
        held = where[p]
        source = jnp.bitwise_xor(held // tile_cols, place[0])
        at = pl.multiple_of((held % tile_cols) * tile, tile)
        out[:, p * tile : (p + 1) * tile] = scr[source, :, pl.ds(at, tile)]


def finish_body(n_row, place, *refs):
    squares, pieces = refs[:n_row], refs[n_row : 2 * n_row]
    scal_first, scal_next, solution, residual = refs[2 * n_row :]
    rows = squares[0].shape[0]
    total = squares[0][...]
    for k in range(1, n_row):
        other = squares[k][...].reshape(n_row, rows // n_row, squares[k].shape[1])
        moved = jnp.stack([other[g ^ k] for g in range(n_row)], axis=0)
        total = total + moved.reshape(total.shape)
    half = rows // (2 * n_row)
    beta_last = jnp.sqrt(both_parts(total[:, 0:1], half))
    alpha_0, beta_0 = scal_first[:, 0:1], scal_first[:, 1:2]
    alpha_1, beta_1 = scal_next[:, 0:1], scal_next[:, 1:2]
    rho = jnp.sqrt(alpha_0 * alpha_0 + beta_1 * beta_1)
    cosine = alpha_0 / rho
    sine = beta_1 / rho
    theta = sine * alpha_1
    rhobar = -cosine * alpha_1
    phi = cosine * beta_0
    phibar = sine * beta_0
    first = phi / rho
    slope = theta / rho
    rho = jnp.sqrt(rhobar * rhobar + beta_last * beta_last)
    second = (rhobar / rho) * phibar / rho
    phibar = (beta_last / rho) * phibar
    weight_0 = (first - second * slope) / alpha_0
    weight_1 = second / alpha_1
    row = jnp.zeros(residual.shape, F32)
    for k in range(n_row):
        held = jnp.bitwise_xor(place[1], k)
        at = pl.multiple_of(held * half, half)
        lo, hi = 2 * half * k, 2 * half * (k + 1)
        v_0 = pieces[k][: 2 * half, :].astype(F32)
        v_1 = pieces[k][2 * half :, :].astype(F32)
        mixed = weight_0[lo:hi] * v_0 + weight_1[lo:hi] * v_1
        for part in range(2):
            solution[part, pl.ds(at, half), :] = mixed[part * half : (part + 1) * half]
        spread = jnp.broadcast_to(phibar[lo : lo + half], (half, residual.shape[1]))
        lane = lax.broadcasted_iota(jnp.int32, spread.shape, 1)
        source = lax.broadcasted_iota(jnp.int32, spread.shape, 0) + at
        row = row + jnp.sum(jnp.where(lane == source, spread, 0.0), axis=0, keepdims=True)
    residual[...] = row


def swap(value, axis, size, mask):
    return lax.ppermute(value, axis, [(j, j ^ mask) for j in range(size)])


def exchange(pieces, axis, size, step):
    got = {k: swap(pieces[k // step], axis, size, k) for k in reversed(range(step, size, step))}
    return [pieces[0]] + [got[k] for k in sorted(got)]


def gather_row(value, size):
    return exchange([value] * size, "row", size, 1)


def gather_col(value, size):
    pieces = []
    for even in exchange([value] * size, "col", size, 2):
        pieces += [even, swap(even, "col", size, 1)]
    return pieces


def on_device(rhs, u_factor, v_factor, ranks, assign):
    n_col, n_row = lax.axis_size("col"), lax.axis_size("row")
    tile_rows, tile_cols, _, tile_size, _ = u_factor.shape
    sources, local = rhs.shape[1], rhs.shape[3]
    rows = 2 * sources
    share = rows // n_row
    width = tile_cols * tile_size
    place = jnp.stack([lax.axis_index("col"), lax.axis_index("row")]).astype(jnp.int32)
    shape = jax.ShapeDtypeStruct
    data_shape, model_shape = shape((rows, local + EXT), BF16), shape((share, width + EXT), BF16)
    chip_shape, pair_shape = shape((n_col // 2, rows, local + EXT), BF16), shape((2 * share, width), BF16)
    scalar_shape = shape((rows, EXT), F32)
    adjoint_scratch = [pltpu.VMEM((tile_rows, rows, tile_size), BF16), pltpu.VMEM((rows, width), F32)]
    forward_scratch = [pltpu.VMEM((rows, width + EXT), BF16), pltpu.VMEM((tile_rows, rows, tile_size), BF16)]

    def forward(pieces):
        keep, send = product(
            functools.partial(forward_body, n_col, n_row),
            place, ranks, u_near, v_near, pieces, [chip_shape] * 2, forward_scratch,
        )
        sums = small(chip_body, [data_shape] * (n_col // 2), keep, swap(send, "col", n_col, 1))
        return exchange(sums, "col", n_col, 2)

    with jax.named_scope("begin"):
        data_0, payload = small(
            functools.partial(begin_body, n_row),
            [shape((rows, local), F32), data_shape],
            place,
            rhs.reshape(2, sources, local),
        )
        pieces = gather_col(payload, n_col)
    with jax.named_scope("adjoint0"):
        *partial_model, u_near, v_near = product(
            functools.partial(adjoint_body, n_col, n_row, True),
            place, ranks, u_factor, v_factor, pieces,
            [model_shape] * n_row + [shape(u_factor.shape, BF16), shape(v_factor.shape, BF16)],
            adjoint_scratch + [pltpu.SemaphoreType.DMA((2, tile_rows))],
            pl.BlockSpec(memory_space=pl.ANY),
        )
        v_hat_0, model_0 = small(
            functools.partial(model_first_body, n_row),
            [shape((share, width), F32), model_shape],
            *exchange(partial_model, "row", n_row, 1),
        )
        pieces = gather_row(model_0, n_row)
    with jax.named_scope("forward0"):
        data_1, payload, scal_first = small(
            functools.partial(data_next_body, n_col, n_row),
            [shape((rows, local), F32), data_shape, scalar_shape],
            data_0,
            *forward(pieces),
        )
        pieces = gather_col(payload, n_col)
    with jax.named_scope("adjoint1"):
        partial_model = product(
            functools.partial(adjoint_body, n_col, n_row, False),
            place, ranks, u_near, v_near, pieces, [model_shape] * n_row, adjoint_scratch,
        )
        model_1, pair = small(
            functools.partial(model_next_body, n_row),
            [model_shape, pair_shape],
            v_hat_0,
            scal_first,
            *exchange(partial_model, "row", n_row, 1),
        )
        pieces = gather_row(model_1, n_row)
    with jax.named_scope("forward1"):
        chip_sums = forward(pieces)

    with jax.named_scope("natural"):
        natural = lax.axis_index("col") * tile_cols + jnp.arange(tile_cols, dtype=jnp.int32)
        positions = jnp.arange(assign.shape[0], dtype=jnp.int32)
        where_held = jnp.sum(
            positions[None, :] * (assign[None, :] == natural[:, None]).astype(jnp.int32), axis=1
        )
        picked = pl.pallas_call(
            functools.partial(pick_body, n_col),
            in_specs=[SMEM, SMEM] + [VMEM] * n_col,
            out_specs=VMEM,
            out_shape=pair_shape,
            scratch_shapes=[pltpu.VMEM((n_col, 2 * share, width), BF16)],
            compiler_params=PARAMS,
        )(place, where_held, *gather_col(pair, n_col))
        blocks = gather_row(picked, n_row)

    with jax.named_scope("last"):
        square, scal_next = small(
            functools.partial(data_last_body, n_col, n_row),
            [scalar_shape, scalar_shape],
            data_1,
            *chip_sums,
        )
        (square,) = small(add_body, [scalar_shape], square, swap(square, "col", n_col, 1))
        (square,) = small(
            add_body, [scalar_shape], *exchange([square] * n_col, "col", n_col, 2)
        )
        solution, residual = small(
            functools.partial(finish_body, n_row),
            [shape((2, sources, width), F32), shape((1, sources), F32)],
            place,
            *gather_row(square, n_row),
            *blocks,
            scal_first,
            scal_next,
        )
    return (solution, residual.reshape(sources))


def solution(mesh):
    in_specs = (
        P(None, None, "row", "col"),
        P("row", "col", None, None, None),
        P("row", "col", None, None, None),
        P("row", "col"),
        P(),
    )
    out_specs = (P(None, None, "col"), P())
    return jax.shard_map(
        on_device, mesh=mesh, in_specs=in_specs, out_specs=out_specs, check_vma=False
    )
```

```python
import functools

import jax
import jax.numpy as jnp
from jax import lax
from jax.experimental import pallas as pl
from jax.experimental.pallas import tpu as pltpu
from jax.sharding import PartitionSpec as P


F32 = jnp.float32
BF16 = jnp.bfloat16
LANES = 128
EXT = 128
VMEM = pl.BlockSpec(memory_space=pltpu.VMEM)
SMEM = pl.BlockSpec(memory_space=pltpu.SMEM)
UNROLL = 16
PARAMS = pltpu.CompilerParams(vmem_limit_bytes=8 * 1024 * 1024)
PRODUCT_PARAMS = pltpu.CompilerParams(vmem_limit_bytes=27 * 1024 * 1024)


def lanes_of(columns, rows):
    lane = lax.broadcasted_iota(jnp.int32, (rows, EXT), 1)
    out = jnp.zeros((rows, EXT), F32)
    for number, column in enumerate(columns):
        rest = column
        for term in range(3):
            part = rest.astype(BF16).astype(F32)
            rest = rest - part
            out = jnp.where(lane == 3 * number + term, part, out)
    return out.astype(BF16)


def column_of(ext, number):
    lane = lax.broadcasted_iota(jnp.int32, ext.shape, 1)
    chosen = (lane >= 3 * number) & (lane < 3 * number + 3)
    return jnp.sum(jnp.where(chosen, ext, 0.0), axis=1, keepdims=True)


def both_parts(column, half):
    real, imag = parts_of(column, half)
    return join(real + imag, real + imag)


def parts_of(raw, half):
    rows, width = raw.shape
    split = raw.reshape(rows // (2 * half), 2, half, width)
    return split[:, 0], split[:, 1]


def join(first, second):
    groups, half, width = first.shape
    return jnp.stack([first, second], axis=1).reshape(groups * 2 * half, width)


def tile_coeff(vec, tile, rank, conj, half):
    k = tile.shape[2]
    raw = jnp.dot(vec, jnp.concatenate([tile[0], tile[1]], axis=1), preferred_element_type=F32)
    rr, ri = parts_of(raw[:, :k], half)
    ir, ii = parts_of(raw[:, k:], half)
    if conj:
        real, imag = rr + ii, ri - ir
    else:
        real, imag = rr - ii, ri + ir
    lane = lax.broadcasted_iota(jnp.int32, real.shape, 2)
    real = jnp.where(lane < rank, real, 0.0)
    imag = jnp.where(lane < rank, imag, 0.0)
    if conj:
        left = jnp.concatenate([join(real, imag), join(imag, -real)], axis=1)
    else:
        left = jnp.concatenate([join(real, imag), join(-imag, real)], axis=1)
    return left.astype(BF16)


def expand(left, tile):
    right = jnp.concatenate([tile[0], tile[1]], axis=1)
    return lax.dot_general(left, right, (((1,), (1,)), ((), ())), preferred_element_type=F32)


def chunks_of(tile_rows):
    chunks, first = [], 0
    while first < tile_rows:
        count = min(1 if first < 2 else 2 if first < 4 else 4, tile_rows - first)
        chunks.append((first, count))
        first += count
    return chunks


def adjoint_body(n_col, n_row, stream, place, ranks, u_ref, v_ref, *refs):
    pieces, outs, rest = refs[:n_col], refs[n_col : n_col + n_row], refs[n_col + n_row :]
    tile_rows, tile_cols, _, tile_size, _ = u_ref.shape
    if stream:
        u_far, v_far, (u_ref, v_ref, d_scr, z_scr, sems) = u_ref, v_ref, rest
        chunks = chunks_of(tile_rows)

        def fetch(number):
            part = pl.ds(chunks[number][0], chunks[number][1])
            return (
                pltpu.make_async_copy(u_far.at[part], u_ref.at[part], sems.at[0, number]),
                pltpu.make_async_copy(v_far.at[part], v_ref.at[part], sems.at[1, number]),
            )

        for number in range(len(chunks)):
            for copy in fetch(number):
                copy.start()
    else:
        d_scr, z_scr = rest
    local = pieces[0].shape[1] - EXT
    width = tile_cols * tile_size
    z_scr[...] = jnp.zeros_like(z_scr)
    for j, piece in enumerate(pieces):
        held = jnp.bitwise_xor(place[0], j)
        if local >= tile_size:
            for w in range(local // tile_size):
                d_scr[held * (local // tile_size) + w] = piece[:, w * tile_size : (w + 1) * tile_size]
        else:
            share = tile_size // local
            d_scr[held // share, :, pl.ds(pl.multiple_of((held % share) * local, local), local)] = piece[:, :local]

    def one_row(i, carry):
        data = d_scr[i]
        half = data.shape[0] // (2 * n_row)
        lefts = [tile_coeff(data, u_ref[i, p], ranks[p, i], True, half) for p in range(tile_cols)]
        for p in range(tile_cols):
            z_scr[:, p * tile_size : (p + 1) * tile_size] += expand(lefts[p], v_ref[i, p])
        return carry

    if stream:
        for number, (first, count) in enumerate(chunks):
            for copy in fetch(number):
                copy.wait()
            for i in range(first, first + count):
                one_row(i, 0)
    else:
        lax.fori_loop(0, tile_rows, one_row, 0, unroll=UNROLL)
    ext = sum(piece[:, local:].astype(F32) for piece in pieces)
    ext = lanes_of([column_of(ext, 0)], ext.shape[0])
    for k, out in enumerate(outs):
        rows = out.shape[0]
        out[:, :width] = z_scr[k * rows : (k + 1) * rows, :].astype(BF16)
        out[:, width:] = ext[k * rows : (k + 1) * rows, :]


def forward_body(n_col, n_row, place, ranks, u_ref, v_ref, *refs):
    pieces, outs, (x_scr, y_scr) = refs[:n_row], refs[n_row : n_row + 2], refs[n_row + 2 :]
    tile_rows, tile_cols, _, tile_size, _ = u_ref.shape
    width = tile_cols * tile_size
    for k, piece in enumerate(pieces):
        rows = piece.shape[0]
        x_scr[k * rows : (k + 1) * rows, :] = piece[...]
    half = x_scr.shape[0] // (2 * n_row)

    def one_row(i, carry):
        lefts = [
            tile_coeff(x_scr[:, p * tile_size : (p + 1) * tile_size], v_ref[i, p], ranks[p, i], False, half)
            for p in range(tile_cols)
        ]
        y_scr[i] = sum(expand(lefts[p], u_ref[i, p]) for p in range(tile_cols)).astype(BF16)
        return carry

    lax.fori_loop(0, tile_rows, one_row, 0, unroll=UNROLL)
    for j in range(n_col):
        out = outs[j % 2].at[j // 2]
        local = out.shape[1] - EXT
        held = jnp.bitwise_xor(place[0], j)
        if local >= tile_size:
            for w in range(local // tile_size):
                out[:, w * tile_size : (w + 1) * tile_size] = y_scr[held * (local // tile_size) + w]
        else:
            share = tile_size // local
            out[:, :local] = y_scr[held // share, :, pl.ds(pl.multiple_of((held % share) * local, local), local)]
        out[:, local:] = x_scr[:, width:]


def forward_half_body(n_row, parity, place, ranks, u_ref, v_ref, *refs):
    pieces, (out, x_scr) = refs[:n_row], refs[n_row:]
    _, tile_cols, _, tile_size, _ = u_ref.shape
    chips, _, wide = out.shape
    per = (wide - EXT) // tile_size
    width = tile_cols * tile_size
    for k, piece in enumerate(pieces):
        rows = piece.shape[0]
        x_scr[k * rows : (k + 1) * rows, :] = piece[...]
    half = x_scr.shape[0] // (2 * n_row)

    def one_chip(k, carry):
        held = jnp.bitwise_xor(place[0], 2 * k + parity)
        for w in range(per):
            i = held * per + w
            lefts = [
                tile_coeff(x_scr[:, p * tile_size : (p + 1) * tile_size], v_ref[i, p], ranks[p, i], False, half)
                for p in range(tile_cols)
            ]
            total = sum(expand(lefts[p], u_ref[i, p]) for p in range(tile_cols))
            out[k, :, w * tile_size : (w + 1) * tile_size] = total.astype(BF16)
        out[k, :, wide - EXT :] = x_scr[:, width:]
        return carry

    lax.fori_loop(0, chips, one_chip, 0, unroll=min(chips, 4))


def product(body, place, ranks, u_factor, v_factor, pieces, out_shapes, scratch, factors=VMEM):
    return pl.pallas_call(
        body,
        in_specs=[SMEM, SMEM, factors, factors] + [VMEM] * len(pieces),
        out_specs=[VMEM] * len(out_shapes),
        out_shape=out_shapes,
        scratch_shapes=scratch,
        compiler_params=PRODUCT_PARAMS,
    )(place, ranks, u_factor, v_factor, *pieces)


def small(body, out_shapes, *args):
    return pl.pallas_call(
        body,
        in_specs=[SMEM if arg.dtype == jnp.int32 else VMEM for arg in args],
        out_specs=[VMEM] * len(out_shapes),
        out_shape=out_shapes,
        compiler_params=PARAMS,
    )(*args)


def total_of(refs, rows, columns):
    return sum(ref[rows, columns].astype(F32) for ref in refs)


def chip_body(keep, other, *outs):
    _, rows, wide = keep.shape
    local = wide - EXT
    ext = keep[0, :, local:].astype(F32) + other[0, :, local:].astype(F32)
    ext = lanes_of([column_of(ext, 0), column_of(ext, 1)], rows)
    for k, out in enumerate(outs):
        out[:, :local] = (keep[k, :, :local].astype(F32) + other[k, :, :local].astype(F32)).astype(BF16)
        out[:, local:] = ext


def begin_body(n_row, place, rhs, data, payload):
    rows, local = data.shape
    half, blocks = rows // (2 * n_row), local // LANES
    for k in range(n_row):
        held = jnp.bitwise_xor(place[1], k)
        for part in range(2):
            at = (2 * k + part) * half
            first = (part * (rows // 2) + held * half) * blocks
            for block in range(blocks):
                lines = pl.ds(first + block, half, stride=blocks) if blocks > 1 else pl.ds(first, half)
                data[at : at + half, block * LANES : (block + 1) * LANES] = rhs[lines, :]
    values = data[...]
    payload[:, :local] = values.astype(BF16)
    payload[:, local:] = lanes_of([jnp.sum(values * values, axis=1, keepdims=True)], rows)


def model_first_body(n_row, *refs):
    pieces, (v_hat, payload) = refs[:n_row], refs[n_row:]
    width = v_hat.shape[1]
    total = total_of(pieces, slice(None), slice(0, width))
    beta2 = both_parts(column_of(total_of(pieces, slice(None), slice(width, None)), 0), total.shape[0] // 2)
    value = total / jnp.sqrt(beta2)
    v_hat[...] = value
    payload[:, :width] = value.astype(BF16)
    payload[:, width:] = lanes_of([beta2, jnp.sum(value * value, axis=1, keepdims=True)], value.shape[0])


def model_next_body(n_row, v_prev, scalars, *refs):
    pieces, (payload, pair) = refs[:n_row], refs[n_row:]
    rows, width = v_prev.shape
    total = total_of(pieces, slice(None), slice(0, width))
    beta2 = both_parts(column_of(total_of(pieces, slice(None), slice(width, None)), 0), total.shape[0] // 2)
    beta = jnp.sqrt(beta2)
    alpha_prev = scalars[:rows, 0:1]
    value = total / beta - (beta / alpha_prev) * v_prev[...]
    payload[:, :width] = value.astype(BF16)
    payload[:, width:] = lanes_of([beta2, jnp.sum(value * value, axis=1, keepdims=True)], rows)
    pair[:rows, :] = v_prev[...].astype(BF16)
    pair[rows:, :] = value.astype(BF16)


def scalars_of(pieces, local, n_col, n_row):
    ext = total_of(pieces, slice(None), slice(local, None))
    beta = jnp.sqrt(column_of(ext, 0) * (1.0 / n_col))
    alpha = jnp.sqrt(both_parts(column_of(ext, 1), ext.shape[0] // (2 * n_row)))
    return alpha, beta


def data_next_body(n_col, n_row, data_prev, *refs):
    pieces, (data, payload, scalars) = refs[: n_col // 2], refs[n_col // 2 :]
    rows, local = data_prev.shape
    alpha, beta = scalars_of(pieces, local, n_col, n_row)
    value = total_of(pieces, slice(None), slice(0, local)) / alpha - (alpha / beta) * data_prev[...]
    data[...] = value
    payload[:, :local] = value.astype(BF16)
    payload[:, local:] = lanes_of([jnp.sum(value * value, axis=1, keepdims=True)], rows)
    lane = lax.broadcasted_iota(jnp.int32, scalars.shape, 1)
    scalars[...] = jnp.where(lane == 0, alpha, beta)


def own_rows(place, rows, share):
    lane = lax.broadcasted_iota(jnp.int32, (rows, LANES), 1)
    row = lax.broadcasted_iota(jnp.int32, (rows, LANES), 0)
    group = jnp.bitwise_xor(row // share, place[1])
    return lane, group * share + row % share


def data_last_body(n_col, n_row, place, data_prev, *refs):
    pieces, (square, scalars) = refs[: n_col // 2], refs[n_col // 2 :]
    rows, local = data_prev.shape
    alpha, beta = scalars_of(pieces, local, n_col, n_row)
    value = total_of(pieces, slice(None), slice(0, local)) / alpha - (alpha / beta) * data_prev[...]
    column = jnp.sum(value * value, axis=1, keepdims=True)
    lane, row = own_rows(place, rows, rows // n_row)
    line = jnp.sum(jnp.where(lane == row, jnp.broadcast_to(column, lane.shape), 0.0), axis=0, keepdims=True)
    square[...] = jnp.broadcast_to(line, square.shape)
    lane = lax.broadcasted_iota(jnp.int32, scalars.shape, 1)
    scalars[...] = jnp.where(lane == 0, alpha, beta)


def add_body(*refs):
    refs[-1][...] = sum(ref[...] for ref in refs[:-1])


def pick_body(n_col, place, where, *refs):
    pieces, (out, scr) = refs[:n_col], refs[n_col:]
    tile_cols = where.shape[0]
    tile = out.shape[1] // tile_cols
    for j in range(n_col):
        scr[j] = pieces[j][...]
    for p in range(tile_cols):
        held = where[p]
        source = jnp.bitwise_xor(held // tile_cols, place[0])
        at = pl.multiple_of((held % tile_cols) * tile, tile)
        out[:, p * tile : (p + 1) * tile] = scr[source, :, pl.ds(at, tile)]


def finish_body(n_row, place, *refs):
    squares, pieces = refs[:n_row], refs[n_row : 2 * n_row]
    scal_first, scal_next, solution, residual = refs[2 * n_row :]
    rows = scal_first.shape[0]
    half = rows // (2 * n_row)
    lane, row = own_rows(place, rows, 2 * half)
    line = total_of(squares, slice(0, 1), slice(None))
    column = jnp.sum(jnp.where(lane == row, jnp.broadcast_to(line, lane.shape), 0.0), axis=1, keepdims=True)
    beta_last = jnp.sqrt(both_parts(column, half))
    alpha_0, beta_0 = scal_first[:, 0:1], scal_first[:, 1:2]
    alpha_1, beta_1 = scal_next[:, 0:1], scal_next[:, 1:2]
    rho = jnp.sqrt(alpha_0 * alpha_0 + beta_1 * beta_1)
    cosine = alpha_0 / rho
    sine = beta_1 / rho
    theta = sine * alpha_1
    rhobar = -cosine * alpha_1
    phi = cosine * beta_0
    phibar = sine * beta_0
    first = phi / rho
    slope = theta / rho
    rho = jnp.sqrt(rhobar * rhobar + beta_last * beta_last)
    second = (rhobar / rho) * phibar / rho
    phibar = (beta_last / rho) * phibar
    weight_0 = (first - second * slope) / alpha_0
    weight_1 = second / alpha_1
    row = jnp.zeros(residual.shape, F32)
    for k in range(n_row):
        held = jnp.bitwise_xor(place[1], k)
        at = pl.multiple_of(held * half, half)
        lo, hi = 2 * half * k, 2 * half * (k + 1)
        v_0 = pieces[k][: 2 * half, :].astype(F32)
        v_1 = pieces[k][2 * half :, :].astype(F32)
        mixed = weight_0[lo:hi] * v_0 + weight_1[lo:hi] * v_1
        for part in range(2):
            solution[part, pl.ds(at, half), :] = mixed[part * half : (part + 1) * half]
        spread = jnp.broadcast_to(phibar[lo : lo + half], (half, residual.shape[1]))
        lane = lax.broadcasted_iota(jnp.int32, spread.shape, 1)
        source = lax.broadcasted_iota(jnp.int32, spread.shape, 0) + at
        row = row + jnp.sum(jnp.where(lane == source, spread, 0.0), axis=0, keepdims=True)
    residual[...] = row


def swap(value, axis, size, mask):
    return lax.ppermute(value, axis, [(j, j ^ mask) for j in range(size)])


def exchange(pieces, axis, size, step):
    got = {}
    for k in reversed(range(step, size, step)):
        got[k] = swap(pieces[k // step], axis, size, k)
    return [pieces[0]] + [got[k] for k in sorted(got)]


def gather_row(value, size):
    return exchange([value] * size, "row", size, 1)


def gather_col(value, size):
    pieces = []
    for even in exchange([value] * size, "col", size, 2):
        pieces += [even, swap(even, "col", size, 1)]
    return pieces


def on_device(rhs, u_factor, v_factor, ranks, assign):
    n_col, n_row = lax.axis_size("col"), lax.axis_size("row")
    tile_rows, tile_cols, _, tile_size, _ = u_factor.shape
    sources, local = rhs.shape[1], rhs.shape[3]
    rows = 2 * sources
    share = rows // n_row
    width = tile_cols * tile_size
    ranks = ranks.T
    place = jnp.stack([lax.axis_index("col"), lax.axis_index("row")]).astype(jnp.int32)
    shape = jax.ShapeDtypeStruct
    data_shape, model_shape = shape((rows, local + EXT), BF16), shape((share, width + EXT), BF16)
    chip_shape, pair_shape = shape((n_col // 2, rows, local + EXT), BF16), shape((2 * share, width), BF16)
    scalar_shape, square_shape = shape((rows, EXT), F32), shape((8, LANES), F32)
    adjoint_scratch = [pltpu.VMEM((tile_rows, rows, tile_size), BF16), pltpu.VMEM((rows, width), F32)]
    forward_scratch = [pltpu.VMEM((rows, width + EXT), BF16), pltpu.VMEM((tile_rows, rows, tile_size), BF16)]

    def forward(pieces, split):
        if local % tile_size or not split:
            keep, send = product(
                functools.partial(forward_body, n_col, n_row),
                place, ranks, u_near, v_near, pieces, [chip_shape] * 2, forward_scratch,
            )
        else:
            send, keep = [
                product(
                    functools.partial(forward_half_body, n_row, parity),
                    place, ranks, u_near, v_near, pieces, [chip_shape], forward_scratch[:1],
                )[0]
                for parity in (1, 0)
            ]
        sums = small(chip_body, [data_shape] * (n_col // 2), keep, swap(send, "col", n_col, 1))
        return exchange(sums, "col", n_col, 2)

    data_0, payload = small(
        functools.partial(begin_body, n_row),
        [shape((rows, local), F32), data_shape],
        place,
        rhs.reshape(rows * local // LANES, LANES),
    )
    pieces = gather_col(payload, n_col)
    *partial_model, u_near, v_near = product(
        functools.partial(adjoint_body, n_col, n_row, True),
        place, ranks, u_factor, v_factor, pieces,
        [model_shape] * n_row + [shape(u_factor.shape, BF16), shape(v_factor.shape, BF16)],
        adjoint_scratch + [pltpu.SemaphoreType.DMA((2, len(chunks_of(tile_rows))))],
        pl.BlockSpec(memory_space=pl.ANY),
    )
    v_hat_0, model_0 = small(
        functools.partial(model_first_body, n_row),
        [shape((share, width), F32), model_shape],
        *exchange(partial_model, "row", n_row, 1),
    )
    pieces = gather_row(model_0, n_row)
    data_1, payload, scal_first = small(
        functools.partial(data_next_body, n_col, n_row),
        [shape((rows, local), F32), data_shape, scalar_shape],
        data_0,
        *forward(pieces, True),
    )
    pieces = gather_col(payload, n_col)
    partial_model = product(
        functools.partial(adjoint_body, n_col, n_row, False),
        place, ranks, u_near, v_near, pieces, [model_shape] * n_row, adjoint_scratch,
    )
    model_1, pair = small(
        functools.partial(model_next_body, n_row),
        [model_shape, pair_shape],
        v_hat_0,
        scal_first,
        *exchange(partial_model, "row", n_row, 1),
    )
    pieces = gather_row(model_1, n_row)
    chip_sums = forward(pieces, False)

    natural = lax.axis_index("col") * tile_cols + jnp.arange(tile_cols, dtype=jnp.int32)
    positions = jnp.arange(assign.shape[0], dtype=jnp.int32)
    where_held = jnp.sum(
        positions[None, :] * (assign[None, :] == natural[:, None]).astype(jnp.int32), axis=1
    )
    held = gather_col(pair, n_col)
    picked = pl.pallas_call(
        functools.partial(pick_body, n_col),
        in_specs=[SMEM, SMEM] + [VMEM] * n_col,
        out_specs=VMEM,
        out_shape=pair_shape,
        scratch_shapes=[pltpu.VMEM((n_col, 2 * share, width), BF16)],
        compiler_params=PARAMS,
    )(place, where_held, *held)
    blocks = gather_row(picked, n_row)

    square, scal_next = small(
        functools.partial(data_last_body, n_col, n_row),
        [square_shape, scalar_shape],
        place,
        data_1,
        *chip_sums,
    )
    (square,) = small(add_body, [square_shape], square, swap(square, "col", n_col, 1))
    (square,) = small(
        add_body, [square_shape], *exchange([square] * n_col, "col", n_col, 2)
    )
    solution, residual = small(
        functools.partial(finish_body, n_row),
        [shape((2, sources, width), F32), shape((1, sources), F32)],
        place,
        *gather_row(square, n_row),
        *blocks,
        scal_first,
        scal_next,
    )
    return (solution, residual.reshape(sources))


def solution(mesh):
    in_specs = (
        P(None, None, "row", "col"),
        P("row", "col", None, None, None),
        P("row", "col", None, None, None),
        P("row", "col"),
        P(),
    )
    out_specs = (P(None, None, "col"), P())

    return jax.shard_map(on_device, mesh=mesh, in_specs=in_specs, out_specs=out_specs, check_vma=False)
```
